32 devices in a mesh: mp: 8 (over y, x, core), hidden: 4 (over z).
Axes of the slice: x: 2, y: 2, z: 4, core: 2. Of those that a mesh axis runs over, the one named last changes fastest.
Arguments:
- states: bfloat16 [512, 16384], P(None, 'mp'), may hold values from -6 to 6
- gate_codes: bfloat16 [16384, 26624], P('mp', 'hidden'), may hold values from -127 to 127, as said below
- gate_scales: float32 [128, 26624], P('mp', 'hidden'), may hold values from 7.8125e-05 to 0.000703125
- up_codes: bfloat16 [16384, 26624], P('mp', 'hidden'), may hold values from -127 to 127, as said below
- up_scales: float32 [128, 26624], P('mp', 'hidden'), may hold values from 7.8125e-05 to 0.000703125
- down_codes: bfloat16 [26624, 16384], P('hidden', 'mp'), may hold values from -127 to 127, as said below
- down_scales: float32 [208, 16384], P('hidden', 'mp'), may hold values from 1.2257258e-05 to 0.000110315326
Outputs:
- output: bfloat16 [512, 16384], P(None, 'mp')
The draws below stay inside these ranges and needn't reach their ends.
Inputs may be any that keep to these rules, and one draw needn't show every extreme that they name: `gate_codes`: whole numbers. `up_codes`: whole numbers. `down_codes`: whole numbers.
All inputs are finite; a program needn't handle non-finite values. Where the reference program divides by a largest or mean magnitude, that divisor is 1e-20 or more.
Results may differ from the reference program's by a relative error of at most 0.02.
Values may be sent and summed in bfloat16 or wider, within the bound.
A program may use at most 256 MiB of HBM per device.

```python
import math
import jax
import jax.numpy as jnp

D = 16384
FF = 26624
BLOCK = 128
ROWS = 512
N_MP = 8
N_HIDDEN = 4


def draw_gate_codes(key, part):
    return jax.random.randint(jax.random.fold_in(key, 11), (D, FF), -127, 128).astype(jnp.float32).astype(jnp.bfloat16)


def draw_up_codes(key, part):
    return jax.random.randint(jax.random.fold_in(key, 23), (D, FF), -127, 128).astype(jnp.float32).astype(jnp.bfloat16)


def draw_down_codes(key, part):
    return jax.random.randint(jax.random.fold_in(key, 37), (FF, D), -127, 128).astype(jnp.float32).astype(jnp.bfloat16)


def steps_of(own_key, extent, shards, low, high):
    loudness, own = 1.0, jax.random.fold_in(own_key, 6)
    for dim, shards_of in shards:
        heights = jnp.exp(jax.random.uniform(jax.random.fold_in(own, dim), (shards_of,), jnp.float32, low / len(shards), high / len(shards)))
        loudness = loudness * jnp.repeat(heights, extent[dim] // shards_of).reshape([-1 if axis == dim else 1 for axis in range(len(extent))])
    return loudness


def centred(rng, dims, deviation, most, split=(), held_as=jnp.bfloat16):
    values = deviation * jax.random.normal(rng, dims, jnp.float32)
    if split:
        values = values * steps_of(rng, dims, split, -0.22, 0.18)
    return jnp.clip(values, -most, most).astype(held_as)


def setup_inputs(seed: int = 0) -> dict:
    arg_keys = jax.random.split(jax.random.key(seed), 8)
    states = centred(arg_keys[0], (ROWS, D), 1.0, 6.0, ((1, 8),))
    gate_codes = draw_gate_codes(jax.random.fold_in(arg_keys[7], 71), 0)
    gate_scales = jnp.clip(jnp.exp(math.log(0.000703125) - 2.1972246 * jax.random.uniform(arg_keys[2], (D // BLOCK, FF), jnp.float32) ** steps_of(arg_keys[2], (D // BLOCK, FF), ((0, 8), (1, 4)), -0.2, 0.2)), 7.812499825377017e-05, 0.000703125)
    up_codes = draw_up_codes(jax.random.fold_in(arg_keys[7], 71), 0)
    up_scales = jnp.clip(jnp.exp(math.log(0.000703125) - 2.1972246 * jax.random.uniform(arg_keys[4], (D // BLOCK, FF), jnp.float32) ** steps_of(arg_keys[4], (D // BLOCK, FF), ((0, 8), (1, 4)), -0.2, 0.2)), 7.812499825377017e-05, 0.000703125)
    down_codes = draw_down_codes(jax.random.fold_in(arg_keys[7], 71), 0)
    down_scales = jnp.clip(jnp.exp(math.log(0.000110315326) - 2.1972246 * jax.random.uniform(arg_keys[6], (FF // BLOCK, D), jnp.float32) ** steps_of(arg_keys[6], (FF // BLOCK, D), ((0, 4), (1, 8)), -0.2, 0.2)), 1.225725827680435e-05, 0.000110315326)
    return dict(states=states, gate_codes=gate_codes, gate_scales=gate_scales, up_codes=up_codes, up_scales=up_scales, down_codes=down_codes, down_scales=down_scales)


epsilon = 1e-6


def dequantize(quantized, scales):
    depth, columns = quantized.shape
    groups = scales.shape[0]
    blocks = quantized.astype(jnp.float32).reshape(groups, depth // groups, columns)
    return (blocks * scales.astype(jnp.float32)[:, None, :]).reshape(depth, columns).astype(jnp.bfloat16)


def encode(values):
    row_count, columns = values.shape
    blocks = values.reshape(row_count, columns // BLOCK, BLOCK)
    maxima = (jnp.max(jnp.abs(blocks), axis=-1) + epsilon).astype(jnp.bfloat16)
    factor = 127.0 / maxima.astype(jnp.float32)
    codes = (blocks * factor[..., None]).astype(jnp.bfloat16)
    return codes.reshape(row_count, columns), maxima


def decode(codes, maxima):
    row_count, columns = codes.shape
    blocks = codes.astype(jnp.float32).reshape(row_count, columns // BLOCK, BLOCK)
    step_size = maxima.astype(jnp.float32) / 127.0
    return (blocks * step_size[..., None]).reshape(row_count, columns)


def reference(states, gate_codes, gate_scales, up_codes, up_scales, down_codes, down_scales):
    piece = D // N_MP
    groups = piece // BLOCK
    gate_sum = jnp.zeros((ROWS, FF), jnp.float32)
    up_sum = jnp.zeros((ROWS, FF), jnp.float32)
    for source in range(N_MP):
        inputs = states[:, source * piece:(source + 1) * piece]
        gate_w = dequantize(gate_codes[source * piece:(source + 1) * piece], gate_scales[source * groups:(source + 1) * groups])
        gate_part = jnp.dot(inputs, gate_w, preferred_element_type=jnp.float32)
        gate_sum = gate_sum + decode(*encode(gate_part))
        up_w = dequantize(up_codes[source * piece:(source + 1) * piece], up_scales[source * groups:(source + 1) * groups])
        up_part = jnp.dot(inputs, up_w, preferred_element_type=jnp.float32)
        up_sum = up_sum + decode(*encode(up_part))
    swiglu = jax.nn.silu(gate_sum) * up_sum
    activation = decode(*encode(swiglu)).astype(jnp.bfloat16)
    width = FF // N_HIDDEN
    wgroups = width // BLOCK
    result = jnp.zeros((ROWS, D), jnp.float32)
    for owner in range(N_HIDDEN):
        down_w = dequantize(down_codes[owner * width:(owner + 1) * width], down_scales[owner * wgroups:(owner + 1) * wgroups])
        result = result + jnp.dot(activation[:, owner * width:(owner + 1) * width], down_w, preferred_element_type=jnp.float32)
    return (result + states.astype(jnp.float32)).astype(jnp.bfloat16)
```

```python
import functools

import jax
import jax.numpy as jnp
from jax import lax
from jax.experimental import pallas as pl
from jax.experimental.pallas import tpu as pltpu
from jax.sharding import PartitionSpec as P

F32, BF16 = jnp.float32, jnp.bfloat16
CHUNKS = 4
PIECES = 4


def plain(i):
    return i


def exchange(x, axis, n, code, bit):
    where = {code(i): i for i in range(n)}
    return lax.ppermute(x, axis, [(i, where[code(i) ^ bit]) for i in range(n)])


def dequant(codes, scales):
    depth, columns = codes.shape
    groups = scales.shape[0]
    blocks = codes.astype(F32).reshape(groups, depth // groups, columns)
    return (blocks * scales.reshape(groups, 1, columns)).reshape(depth, columns).astype(BF16)


def permute_kernel(n, me_ref, x_ref, o_ref):
    for i in range(n):
        o_ref[i] = x_ref[i ^ me_ref[0]]


def permute_rows(x, me, n):
    rows, columns = x.shape
    tile = columns // 2
    spec = pl.BlockSpec((n, rows // n, tile), lambda j, m: (0, 0, j))
    return pl.pallas_call(
        functools.partial(permute_kernel, n),
        out_shape=jax.ShapeDtypeStruct((n, rows // n, columns), x.dtype),
        grid_spec=pltpu.PrefetchScalarGridSpec(num_scalar_prefetch=1, grid=(2,), in_specs=[spec], out_specs=spec),
        cost_estimate=pl.CostEstimate(flops=0, bytes_accessed=4 * rows * columns, transcendentals=0),
    )(me, x.reshape(n, rows // n, columns)).reshape(rows, columns)


def up_kernel(x_ref, gc, gs, uc, us, g_keep, g_send, u_keep, u_send):
    for codes, scales, keep, send in ((gc, gs, g_keep, g_send), (uc, us, u_keep, u_send)):
        part = jnp.dot(x_ref[...], dequant(codes[...], scales[...]), preferred_element_type=F32).astype(BF16)
        half, rb, tile = keep.shape
        part = part.reshape(half, 2, rb, tile)
        keep[...] = part[:, 0]
        send[...] = part[:, 1]


def up_call(x, gc, gs, uc, us, first, count, tile, n):
    rows, depth = x.shape
    groups = gs.shape[0]
    rb = rows // n
    w = pl.BlockSpec((depth, tile), lambda j: (0, first + j))
    s = pl.BlockSpec((groups, tile), lambda j: (0, first + j))
    o = pl.BlockSpec((n // 2, rb, tile), lambda j: (0, 0, j))
    shape = jax.ShapeDtypeStruct((n // 2, rb, count * tile), BF16)
    return pl.pallas_call(
        up_kernel,
        out_shape=[shape] * 4,
        grid=(count,),
        in_specs=[pl.BlockSpec((rows, depth), lambda j: (0, 0)), w, s, w, s],
        out_specs=[o] * 4,
        compiler_params=pltpu.CompilerParams(vmem_limit_bytes=56 << 20),
        cost_estimate=pl.CostEstimate(
            flops=4 * rows * depth * count * tile, bytes_accessed=4 * depth * count * tile, transcendentals=0
        ),
    )(x, gc, gs, uc, us)


def down_kernel(count, first, last, z_ref, x_ref, *refs):
    codes, scales, rest = refs[:count], refs[count : 2 * count], refs[2 * count :]
    out = rest[-1]
    w = jnp.concatenate([dequant(codes[k][...], scales[k][...]) for k in range(count)], axis=0)
    total = jnp.dot(x_ref[...], w, preferred_element_type=F32)
    if not first:
        total = total + rest[0][0]
    out[0] = total.astype(out.dtype)


def down_call(x, dc, ds, total, z, first, count, tile, nz, last):
    rows = x.shape[0]
    columns = dc.shape[1]
    tn = columns // nz
    groups = tile // (dc.shape[0] // ds.shape[0])
    ws = [pl.BlockSpec((tile, tn), lambda j, z, k=k: (first + k, j ^ z[0])) for k in range(count)]
    ss = [pl.BlockSpec((groups, 1, tn), lambda j, z, k=k: (first + k, 0, j ^ z[0])) for k in range(count)]
    o = pl.BlockSpec((1, rows, tn), lambda j, z: (j, 0, 0))
    extra = [] if total is None else [total]
    return pl.pallas_call(
        functools.partial(down_kernel, count, total is None, last),
        out_shape=jax.ShapeDtypeStruct((nz, rows, tn), BF16 if last else F32),
        grid_spec=pltpu.PrefetchScalarGridSpec(
            num_scalar_prefetch=1,
            grid=(nz,),
            in_specs=[pl.BlockSpec((rows, count * tile), lambda j, z: (0, 0))] + ws + ss + [o] * len(extra),
            out_specs=o,
        ),
        compiler_params=pltpu.CompilerParams(vmem_limit_bytes=56 << 20),
        cost_estimate=pl.CostEstimate(
            flops=2 * rows * columns * count * tile, bytes_accessed=2 * columns * count * tile, transcendentals=0
        ),
    )(z, x, *([dc] * count), *([ds] * count), *extra)


def place_kernel(n, ids_ref, x_ref, o_ref):
    rb = o_ref.shape[0] // n
    for i in range(n):
        o_ref[i * rb : (i + 1) * rb] = x_ref[0, i ^ ids_ref[0]]


def place(x, ids, n):
    nz, rows, tn = x.shape
    rb = rows // n
    return pl.pallas_call(
        functools.partial(place_kernel, n),
        out_shape=jax.ShapeDtypeStruct((rows, nz * tn), x.dtype),
        grid_spec=pltpu.PrefetchScalarGridSpec(
            num_scalar_prefetch=1,
            grid=(nz,),
            in_specs=[pl.BlockSpec((1, n, rb, tn), lambda j, ids: (j ^ ids[1], 0, 0, 0))],
            out_specs=pl.BlockSpec((rows, tn), lambda j, ids: (0, j)),
        ),
    )(ids, x.reshape(nz, n, rb, tn))


def without(i, bit):
    return [p for p in i if not p & bit], [p for p in i if p & bit]


def scatter_sum(terms, axis, n, code, bits, marks=None):
    positions = list(range(n))
    for bit in bits:
        kept, sent = without(positions, bit)
        if isinstance(terms, tuple):
            keep, send = terms
            terms = [{p: keep[i] for i, p in enumerate(kept)}]
        else:
            send = jnp.stack([sum(t[p].astype(F32) for t in terms).astype(BF16) for p in sent])
        got = exchange(send, axis, n, code, bit)
        terms = terms + [{p: got[i] for i, p in enumerate(kept)}]
        if marks is not None:
            marks.append(got)
        positions = kept
    return sum(t[0].astype(F32) for t in terms)


def gather(x, axis, n, code, bits):
    held, positions = x[None], [0]
    for bit in bits:
        got = exchange(held, axis, n, code, bit)
        held = jnp.concatenate([held, got])
        positions = positions + [p ^ bit for p in positions]
    if positions != sorted(positions):
        held = jnp.stack([held[positions.index(p)] for p in range(n)])
    return held


def body(sizes, states, gc, gs, uc, us, dc, ds):
    n, nz = sizes
    rows = states.shape[0]
    hidden = gc.shape[1]
    me = lax.axis_index("mp").astype(jnp.int32)
    z = lax.axis_index("hidden").astype(jnp.int32)
    zc = z
    tile = next(t for t in (512, 256, 128) if hidden % t == 0)
    tiles = hidden // tile
    counts = [tiles // CHUNKS + (c < tiles % CHUNKS) for c in range(CHUNKS)]
    bits = [1 << i for i in range(n.bit_length() - 1)]
    order_a, order_b = bits, bits[:1] + bits[:0:-1]
    zbits = [1 << i for i in range(nz.bit_length() - 1)]

    x = permute_rows(states, me[None], n)
    ds3 = ds.reshape(ds.shape[0], 1, ds.shape[1])
    total = None
    first = 0
    starts = []
    for count in counts:
        starts.append(first)
        first += count
    acts = []
    marks = []
    for i, (first, count) in enumerate(zip(starts, counts)):
        waits = [m[i - 2 - c] for c in range(i - 1) for m in marks[c] if len(m) > i - 2 - c]
        if waits:
            x_now, *_ = lax.optimization_barrier((x, *waits))
        else:
            x_now = x
        marks.append(([], []))
        g_keep, g_send, u_keep, u_send = up_call(x_now, gc, gs, uc, us, first, count, tile, n)
        g = scatter_sum((g_keep, g_send), "mp", n, plain, order_a, marks[i][0])
        u = scatter_sum((u_keep, u_send), "mp", n, plain, order_b, marks[i][1])
        act = (jax.nn.silu(g) * u).astype(BF16)
        half = act.shape[1] // 2
        acts.append(
            jnp.concatenate(
                [
                    gather(act[:, :half], "mp", n, plain, order_a[::-1]),
                    gather(act[:, half:], "mp", n, plain, order_b[::-1]),
                ],
                axis=2,
            ).reshape(rows, count * tile)
        )
    for i, (first, count) in enumerate(zip(starts, counts)):
        total = down_call(acts[i], dc, ds3, total, zc[None], first, count, tile, nz, i == CHUNKS - 1)

    tn = dc.shape[1] // nz
    own = lax.dynamic_slice(x, (0, zc * tn), (rows, tn)).astype(F32)
    done = []
    step = rows // PIECES
    for h in range(PIECES):
        cut = slice(h * step, (h + 1) * step)
        mine = scatter_sum([{p: total[p, cut] for p in range(nz)}], "hidden", nz, plain, zbits)
        mine = (mine + own[cut]).astype(BF16)
        done.append(gather(mine, "hidden", nz, plain, zbits[::-1]))
    return place(jnp.concatenate(done, axis=1), jnp.stack([me, zc]), n)


def solution(mesh):
    in_specs = (
        P(None, "mp"),
        P("mp", "hidden"),
        P("mp", "hidden"),
        P("mp", "hidden"),
        P("mp", "hidden"),
        P("hidden", "mp"),
        P("hidden", "mp"),
    )
    sizes = (mesh.shape["mp"], mesh.shape["hidden"])
    return jax.shard_map(
        functools.partial(body, sizes), mesh=mesh, in_specs=in_specs, out_specs=P(None, "mp"), check_vma=False
    )
```
